32 devices in a mesh: patch: 8 (over z, x), rep: 4 (over y, core).
Axes of the slice: x: 2, y: 2, z: 4, core: 2. Of those that a mesh axis runs over, the one named last changes fastest.
Arguments:
- node_latents: bfloat16 [4, 3072, 512], P('rep', 'patch'), may hold values from -6 to 6
- edge_latents: bfloat16 [4, 10240, 512], P('rep', 'patch'), may hold values from -6 to 6
- targets: bfloat16 [4, 3072, 128], P('rep', 'patch'), may hold values from -6 to 6
- edge_weight_in: bfloat16 [1536, 512], replicated, may hold values from -0.15625 to 0.15625
- edge_weight_out: bfloat16 [512, 512], replicated, may hold values from -0.25 to 0.25
- node_weight_in: bfloat16 [1024, 512], replicated, may hold values from -0.1875 to 0.1875
- node_weight_out: bfloat16 [512, 512], replicated, may hold values from -0.25 to 0.25
- readout_weight: bfloat16 [512, 128], replicated, may hold values from -0.25 to 0.25
- send_rows: int32 [8, 96], P('patch'), may hold values from 0 to 383, as said below
- far_rows: int32 [8, 8], P('patch'), may hold values from 0 to 383, as said below
- edge_sender: int32 [10240], P('patch'), may hold values from 0 to 487
- edge_receiver: int32 [10240], P('patch'), may hold values from 0 to 383
- edge_count: int32 [8], P('patch'), may hold values from 80 to 1280, as said below
- land_mask: int32 [3072], P('patch'), may hold values 0 or 1
- lat_band: int32 [3072], P('patch'), may hold values from 0 to 720
Outputs:
- node_grad: bfloat16 [4, 3072, 512], P('rep', 'patch')
- edge_grad: bfloat16 [4, 10240, 512], P('rep', 'patch')
- grad_edge_in: float32 [1536, 512], P('patch')
- grad_edge_out: float32 [512, 512], P('patch')
- grad_node_in: float32 [1024, 512], P('patch')
- grad_node_out: float32 [512, 512], P('patch')
- grad_readout: float32 [512, 128], P('patch')
The draws below stay inside these ranges and needn't reach their ends.
Inputs may be any that keep to these rules, and one draw needn't show every extreme that they name: `send_rows`: the 16 entries of a patch for one neighbour are distinct. `far_rows`: each patch sends exactly one node to every patch (itself included). `edge_count`: some patch has all 1280 edges live.
All inputs are finite; a program needn't handle non-finite values. No bound on the sum of `land_mask` on one device may be relied on, other than what follows from the above.
Results may differ from the reference program's by a relative error of at most 0.012.
Values may be sent and summed in bfloat16 or wider, within the bound.
No kernel may reach another device: no remote copies, remote signals or barrier semaphores. Data moves between devices by JAX's collectives and lax.ppermute only.
A program may use at most 128 MiB of HBM per device.

```python
import jax
import jax.numpy as jnp
from jax import lax

D = 512
VARS = 128
OCEAN = 32
BANDS = 721
NODE_DEV = 384
EDGE_DEV = 1280
SLOT = 16
FAR = 1
PATCHES = 8
REPS = 4
NODES = 3072
EDGES = 10240


def draw_send_rows(key, part):
    patches = EDGES // EDGE_DEV
    scores = jax.random.randint(key, (patches, 6, NODE_DEV), 0, 1 << 16) * NODE_DEV + jnp.arange(NODE_DEV, dtype=jnp.int32)
    order = jnp.argsort(scores, axis=-1, stable=True)[:, :, :SLOT]
    return order.reshape(patches, 6 * SLOT).astype(jnp.int32)


def draw_far_rows(key, part):
    patches = EDGES // EDGE_DEV
    scores = jax.random.randint(key, (patches, patches, NODE_DEV), 0, 1 << 16) * NODE_DEV + jnp.arange(NODE_DEV, dtype=jnp.int32)
    order = jnp.argsort(scores, axis=-1, stable=True)[:, :, :FAR]
    return order.reshape(patches, patches * FAR).astype(jnp.int32)


def draw_edge_sender(key, part):
    patches = EDGES // EDGE_DEV
    kind = jax.random.randint(jax.random.fold_in(key, 1), (EDGES,), 0, 100)
    local = jax.random.randint(jax.random.fold_in(key, 2), (EDGES,), 0, NODE_DEV)
    near = NODE_DEV + jax.random.randint(jax.random.fold_in(key, 3), (EDGES,), 0, 6 * SLOT)
    far = NODE_DEV + 6 * SLOT + jax.random.randint(jax.random.fold_in(key, 4), (EDGES,), 0, FAR * patches)
    return jnp.where(kind < 72, local, jnp.where(kind < 88, near, far)).astype(jnp.int32)


def draw_edge_count(key, part):
    patches = EDGES // EDGE_DEV
    counts = jax.random.randint(key, (patches,), EDGE_DEV // 16, EDGE_DEV + 1)
    fullest = jax.random.randint(jax.random.fold_in(key, 7), (), 0, patches)
    return jnp.where(jnp.arange(patches) == fullest, EDGE_DEV, counts).astype(jnp.int32)


def with_ends(entries, own_key, least, high):
    dims = entries.shape
    spot = [jax.random.randint(jax.random.fold_in(own_key, axis), (), 0, dims[axis]) for axis in range(len(dims))]
    entries = entries.at[tuple(spot)].set(least)
    longest = dims.index(max(dims))
    spot[longest] = (spot[longest] + 1) % dims[longest]
    return entries.at[tuple(spot)].set(high)


def block_levels(rng, extent, pieces, low, high):
    def one(position, parts):
        draws = jax.random.uniform(jax.random.fold_in(jax.random.fold_in(rng, 6), position), (parts,), jnp.float32, low / len(pieces), high / len(pieces))
        return jnp.repeat(jnp.exp(draws), extent[position] // parts).reshape((-1,) + (1,) * (len(extent) - position - 1))

    factor_of = one(*pieces[0])
    for cut in pieces[1:]:
        factor_of = factor_of * one(*cut)
    return factor_of


def normal_values(stream_key, dims, scale, most, split=(), kind=jnp.bfloat16):
    entries = scale * jax.random.normal(stream_key, dims, jnp.float32)
    if split:
        entries = entries * block_levels(stream_key, dims, split, -0.22, 0.18)
    return jnp.clip(entries, -most, most).astype(kind)


def setup_inputs(seed: int = 0) -> dict:
    key_of = jax.random.split(jax.random.key(seed), 16)
    node_latents = normal_values(key_of[0], (REPS, NODES, D), 1.0, 6.0, ((0, 4), (1, 8)))
    edge_latents = normal_values(key_of[1], (REPS, EDGES, D), 1.0, 6.0, ((0, 4), (1, 8)))
    targets = normal_values(key_of[2], (REPS, NODES, VARS), 1.0, 6.0, ((0, 4), (1, 8)))
    edge_weight_in = normal_values(key_of[3], (3 * D, D), (3 * D) ** -0.5, 0.15625)
    edge_weight_out = normal_values(key_of[4], (D, D), D ** -0.5, 0.25)
    node_weight_in = normal_values(key_of[5], (2 * D, D), (2 * D) ** -0.5, 0.1875)
    node_weight_out = normal_values(key_of[6], (D, D), D ** -0.5, 0.25)
    readout_weight = normal_values(key_of[7], (D, VARS), D ** -0.5, 0.25)
    send_rows = draw_send_rows(jax.random.fold_in(key_of[15], 71), 0)
    far_rows = draw_far_rows(jax.random.fold_in(key_of[15], 71), 0)
    edge_sender = draw_edge_sender(jax.random.fold_in(key_of[15], 71), 0)
    edge_receiver = with_ends(jax.random.randint(key_of[11], (EDGES,), 0, NODE_DEV), jax.random.fold_in(key_of[11], 1), 0, NODE_DEV - 1).astype(jnp.int32)
    edge_count = draw_edge_count(jax.random.fold_in(key_of[15], 71), 0)
    land_mask = with_ends((jax.random.randint(key_of[13], (NODES,), 0, 10) < 3).astype(jnp.int32), jax.random.fold_in(key_of[13], 1), 0, 1)
    lat_band = with_ends(jax.random.randint(key_of[14], (NODES,), 0, BANDS), jax.random.fold_in(key_of[14], 1), 0, BANDS - 1).astype(jnp.int32)
    return {"node_latents": node_latents, "edge_latents": edge_latents, "targets": targets, "edge_weight_in": edge_weight_in, "edge_weight_out": edge_weight_out, "node_weight_in": node_weight_in, "node_weight_out": node_weight_out, "readout_weight": readout_weight, "send_rows": send_rows, "far_rows": far_rows, "edge_sender": edge_sender, "edge_receiver": edge_receiver, "edge_count": edge_count, "land_mask": land_mask, "lat_band": lat_band}


def normalize(values):
    average = lax.optimization_barrier(jnp.mean(values, axis=-1, keepdims=True))
    centred = values - average
    variance = lax.optimization_barrier(jnp.mean(centred * centred, axis=-1, keepdims=True))
    inverse = lax.rsqrt(variance + 1e-05)
    return (centred * inverse, inverse)

def norm_back(gradient, normed, inverse):
    first = lax.optimization_barrier(jnp.mean(gradient, axis=-1, keepdims=True))
    second = lax.optimization_barrier(jnp.mean(gradient * normed, axis=-1, keepdims=True))
    return inverse * (gradient - first - normed * second)

def silu_grad(values):
    logistic = jax.nn.sigmoid(values)
    return logistic * (1.0 + values * (1.0 - logistic))

def product(left, right):
    return jnp.dot(left, right, preferred_element_type=jnp.float32)

def product_left(left, right):
    return jnp.dot(left.T, right, preferred_element_type=jnp.float32)

def product_right(left, right):
    return jnp.dot(left, right.T, preferred_element_type=jnp.float32)

def reference(node_latents, edge_latents, targets, edge_weight_in, edge_weight_out, node_weight_in, node_weight_out, readout_weight, send_rows, far_rows, edge_sender, edge_receiver, edge_count, land_mask, lat_band):
    positions = jnp.arange(EDGES, dtype=jnp.int32)
    device = (positions // EDGE_DEV).astype(jnp.int32)
    near_total = 6 * SLOT
    offset = jnp.maximum(edge_sender - NODE_DEV, 0).astype(jnp.int32)
    near_index = jnp.minimum(offset, near_total - 1).astype(jnp.int32)
    neighbour = (near_index // SLOT).astype(jnp.int32)
    distance = ((neighbour // 2 + 1) * (1 - 2 * (neighbour % 2))).astype(jnp.int32)
    near_patch = ((device - distance + PATCHES) % PATCHES).astype(jnp.int32)
    near_node = near_patch * NODE_DEV + send_rows[near_patch, near_index]
    far_index = jnp.maximum(offset - near_total, 0).astype(jnp.int32)
    far_patch = jnp.minimum(far_index // FAR, PATCHES - 1).astype(jnp.int32)
    far_node = far_patch * NODE_DEV + far_rows[far_patch, device * FAR + far_index % FAR]
    remote = jnp.where(offset < near_total, near_node, far_node)
    senders = jnp.where(edge_sender < NODE_DEV, device * NODE_DEV + edge_sender, remote).astype(jnp.int32)
    receivers = (device * NODE_DEV + edge_receiver).astype(jnp.int32)
    alive_mask = (positions % EDGE_DEV < edge_count[device]).astype(jnp.float32)[:, None]
    latitude = -0.5 * jnp.pi + (lat_band.astype(jnp.float32) + 0.5) * (jnp.pi / BANDS)
    area_weight = jnp.cos(latitude)[:, None]
    channel = jnp.arange(VARS, dtype=jnp.int32)
    keep_mask = jnp.where((channel[None, :] < OCEAN) & (land_mask[:, None] == 1), 0.0, 1.0).astype(jnp.float32)
    loss_weight = area_weight * keep_mask
    sums = [jnp.zeros(w.shape, jnp.float32) for w in (edge_weight_in, edge_weight_out, node_weight_in, node_weight_out, readout_weight)]
    node_grads = []
    edge_grads = []
    for replica in range(REPS):
        node_rows = node_latents[replica]
        edge_rows = edge_latents[replica]
        stacked = jnp.concatenate([node_rows[senders], node_rows[receivers], edge_rows], axis=1)
        edge_pre = product(stacked, edge_weight_in)
        edge_hidden = jax.nn.silu(edge_pre).astype(jnp.bfloat16)
        edge_normed, edge_inverse = normalize(product(edge_hidden, edge_weight_out))
        message = (edge_normed * alive_mask).astype(jnp.bfloat16)
        aggregate = jax.ops.segment_sum(message.astype(jnp.float32), receivers, num_segments=NODES).astype(jnp.bfloat16)
        node_input = jnp.concatenate([node_rows, aggregate], axis=1)
        node_pre = product(node_input, node_weight_in)
        node_hidden = jax.nn.silu(node_pre).astype(jnp.bfloat16)
        node_normed, node_inverse = normalize(product(node_hidden, node_weight_out))
        updated = (node_rows.astype(jnp.float32) + node_normed).astype(jnp.bfloat16)
        predicted = product(updated, readout_weight)
        pred_grad = (loss_weight * (predicted - targets[replica].astype(jnp.float32))).astype(jnp.bfloat16)
        updated_grad = product_right(pred_grad, readout_weight)
        node_z_grad = norm_back(updated_grad, node_normed, node_inverse).astype(jnp.bfloat16)
        node_pre_grad = (product_right(node_z_grad, node_weight_out) * silu_grad(node_pre)).astype(jnp.bfloat16)
        input_grad = product_right(node_pre_grad, node_weight_in)
        message_grad = input_grad[:, D:][receivers] * alive_mask
        edge_z_grad = norm_back(message_grad, edge_normed, edge_inverse).astype(jnp.bfloat16)
        edge_pre_grad = (product_right(edge_z_grad, edge_weight_out) * silu_grad(edge_pre)).astype(jnp.bfloat16)
        stacked_grad = product_right(edge_pre_grad, edge_weight_in)
        sender_grad = stacked_grad[:, :D].astype(jnp.bfloat16).astype(jnp.float32)
        receiver_grad = stacked_grad[:, D:2 * D].astype(jnp.bfloat16).astype(jnp.float32)
        edge_grads.append(stacked_grad[:, 2 * D:].astype(jnp.bfloat16))
        total = updated_grad + input_grad[:, :D]
        total = total + jax.ops.segment_sum(sender_grad, senders, num_segments=NODES)
        total = total + jax.ops.segment_sum(receiver_grad, receivers, num_segments=NODES)
        node_grads.append(total.astype(jnp.bfloat16))
        sums[0] = sums[0] + product_left(stacked, edge_pre_grad)
        sums[1] = sums[1] + product_left(edge_hidden, edge_z_grad)
        sums[2] = sums[2] + product_left(node_input, node_pre_grad)
        sums[3] = sums[3] + product_left(node_hidden, node_z_grad)
        sums[4] = sums[4] + product_left(updated, pred_grad)
    factor = 1.0 / (NODES * REPS)
    return (jnp.stack(node_grads), jnp.stack(edge_grads), sums[0] * factor, sums[1] * factor, sums[2] * factor, sums[3] * factor, sums[4] * factor)
```

```python
import jax
import jax.numpy as jnp
from jax import lax
from jax.sharding import PartitionSpec as P

OCEAN = 32
BANDS = 721
OFFSETS = (1, -1, 2, -2, 3, -3)
BF = jnp.bfloat16
F32 = jnp.float32


def normalize(values):
    average = jnp.mean(values, axis=-1, keepdims=True)
    centred = values - average
    variance = jnp.mean(centred * centred, axis=-1, keepdims=True)
    inverse = lax.rsqrt(variance + 1e-05)
    return (centred * inverse, inverse)


def norm_back(gradient, normed, inverse):
    first = jnp.mean(gradient, axis=-1, keepdims=True)
    second = jnp.mean(gradient * normed, axis=-1, keepdims=True)
    return inverse * (gradient - first - normed * second)


def silu_grad(values):
    logistic = jax.nn.sigmoid(values)
    return logistic * (1.0 + values * (1.0 - logistic))


def product(left, right):
    return jnp.dot(left, right, preferred_element_type=F32)


def product_left(left, right):
    return lax.dot_general(left, right, (((0,), (0,)), ((), ())), preferred_element_type=F32)


def product_right(left, right):
    return lax.dot_general(left, right, (((1,), (1,)), ((), ())), preferred_element_type=F32)


def swap(x, axis, mask):
    peers = lax.axis_size(axis)
    return lax.ppermute(x, axis, [(i, i ^ mask) for i in range(peers)])


def halves(x, bit, dim):
    size = x.shape[dim] // 2
    low = lax.slice_in_dim(x, 0, size, axis=dim)
    high = lax.slice_in_dim(x, size, 2 * size, axis=dim)
    upper = bit == 1
    return jnp.where(upper, high, low), jnp.where(upper, low, high).astype(BF)


def masks_of(size):
    return [1 << k for k in range(size.bit_length() - 1)]


def reduce_step(x, axis, mask, dim):
    bit = (lax.axis_index(axis) // mask) % 2
    keep, send = halves(x, bit, dim)
    return keep, send


def reduce_rows(x):
    patches = lax.axis_size("patch")
    replicas = lax.axis_size("rep")
    rep_masks = masks_of(replicas)
    patch_masks = masks_of(patches)
    rows = x.shape[1]
    order = sorted(range(patches), key=lambda q: int(format(q, f"0{len(patch_masks)}b")[::-1], 2))
    x = jnp.concatenate([x[q : q + 1] for q in order], axis=0)
    lane_bits = list(rep_masks)
    if lane_bits:
        keep, send = reduce_step(x, "rep", lane_bits[0], 2)
        x = keep + swap(send, "rep", lane_bits[0]).astype(F32)
        lane_bits = lane_bits[1:]
    rest = list(patch_masks)
    if lane_bits and rest:
        first = rows // 2 // 16 * 16
        a, b = x[:, :first], x[:, first:]
        m, n = lane_bits[0], rest[0]
        ka, sa = reduce_step(a, "rep", m, 2)
        kb, sb = reduce_step(b, "patch", n, 0)
        ra, rb = swap(sa, "rep", m), swap(sb, "patch", n)
        a, b = ka + ra.astype(F32), kb + rb.astype(F32)
        ka, sa = reduce_step(a, "patch", n, 0)
        kb, sb = reduce_step(b, "rep", m, 2)
        ra, rb = swap(sa, "patch", n), swap(sb, "rep", m)
        x = jnp.concatenate([ka + ra.astype(F32), kb + rb.astype(F32)], axis=1)
        lane_bits, rest = lane_bits[1:], rest[1:]
    for m in lane_bits:
        keep, send = reduce_step(x, "rep", m, 2)
        x = keep + swap(send, "rep", m).astype(F32)
    for n in rest:
        keep, send = reduce_step(x, "patch", n, 0)
        x = keep + swap(send, "patch", n).astype(F32)
    x = x[0].astype(BF)
    for m in reversed(rep_masks):
        other = swap(x, "rep", m)
        upper = (lax.axis_index("rep") // m) % 2 == 1
        x = jnp.where(upper, jnp.concatenate([other, x], axis=1), jnp.concatenate([x, other], axis=1))
    return x.astype(F32)


def body(
    node_latents,
    edge_latents,
    targets,
    edge_weight_in,
    edge_weight_out,
    node_weight_in,
    node_weight_out,
    readout_weight,
    send_rows,
    far_rows,
    edge_sender,
    edge_receiver,
    edge_count,
    land_mask,
    lat_band,
):
    width = node_latents.shape[2]
    nodes = node_latents.shape[1]
    edges = edge_latents.shape[1]
    patches = lax.axis_size("patch")
    replicas = lax.axis_size("rep")
    here = lax.axis_index("patch")
    slot = send_rows.shape[1] // 6
    far = far_rows.shape[1] // patches
    slots = -(-(slot + far) // 8) * 8
    node_rows = node_latents[0]
    edge_rows = edge_latents[0]
    target = targets[0].astype(F32)
    node_ids = lax.iota(jnp.int32, nodes)

    peers = lax.iota(jnp.int32, patches)
    offsets = jnp.array(OFFSETS, jnp.int32)
    hit = ((peers[:, None] - here - offsets[None, :]) % patches == 0)[:, :, None]
    near = jnp.sum(jnp.where(hit, send_rows[0].reshape(1, 6, slot) + 1, 0), axis=1) - 1
    fill = jnp.full((patches, slots - slot - far), -1, jnp.int32)
    owned = jnp.concatenate([near, far_rows[0].reshape(patches, far), fill], axis=1)
    owned = owned.reshape(patches * slots)
    pick = (owned[:, None] == node_ids[None, :]).astype(BF)
    outgoing = product(pick, node_rows).astype(BF).reshape(patches, slots, width)
    incoming = lax.all_to_all(outgoing, "patch", split_axis=0, concat_axis=0, tiled=True)
    incoming = incoming.reshape(patches * slots, width)

    beyond = edge_sender - nodes
    k = beyond // slot
    away = (k // 2 + 1) * (1 - 2 * (k % 2))
    near_at = ((here - away) % patches) * slots + beyond % slot
    distant = beyond - 6 * slot
    far_at = (distant // far) * slots + slot + distant % far
    halo_at = jnp.where(beyond < 0, -1, jnp.where(beyond < 6 * slot, near_at, far_at))
    halo_ids = lax.iota(jnp.int32, patches * slots)
    from_own = (edge_sender[:, None] == node_ids[None, :]).astype(BF)
    from_halo = (halo_at[:, None] == halo_ids[None, :]).astype(BF)
    to_own = (edge_receiver[:, None] == node_ids[None, :]).astype(BF)

    weight_s = edge_weight_in[:width]
    weight_r = edge_weight_in[width : 2 * width]
    weight_e = edge_weight_in[2 * width :]
    sent_part = product(node_rows, weight_s).astype(BF)
    received_part = product(node_rows, weight_r).astype(BF)
    halo_part = product(incoming, weight_s).astype(BF)
    positions = lax.iota(jnp.int32, edges)
    alive = (positions < edge_count[0]).astype(F32)[:, None]
    edge_pre = (
        product(jnp.concatenate([from_own, to_own], axis=1), jnp.concatenate([sent_part, received_part], axis=0))
        + product(edge_rows, weight_e)
        + product(from_halo, halo_part)
    )
    edge_hidden = jax.nn.silu(edge_pre).astype(BF)
    edge_normed, edge_inverse = normalize(product(edge_hidden, edge_weight_out))
    message = (edge_normed * alive).astype(BF)
    aggregate = product_left(to_own, message).astype(BF)
    node_input = jnp.concatenate([node_rows, aggregate], axis=1)
    node_pre = product(node_input, node_weight_in)
    node_hidden = jax.nn.silu(node_pre).astype(BF)
    node_normed, node_inverse = normalize(product(node_hidden, node_weight_out))
    updated = (node_rows.astype(F32) + node_normed).astype(BF)
    predicted = product(updated, readout_weight)
    latitude = -0.5 * jnp.pi + (lat_band.astype(F32) + 0.5) * (jnp.pi / BANDS)
    channel = lax.iota(jnp.int32, readout_weight.shape[1])
    keep_mask = jnp.where((channel[None, :] < OCEAN) & (land_mask[:, None] == 1), 0.0, 1.0)
    loss_weight = jnp.cos(latitude)[:, None] * keep_mask
    pred_grad = (loss_weight * (predicted - target)).astype(BF)
    updated_grad = product_right(pred_grad, readout_weight)
    node_z_grad = norm_back(updated_grad, node_normed, node_inverse).astype(BF)
    node_pre_grad = (product_right(node_z_grad, node_weight_out) * silu_grad(node_pre)).astype(BF)
    input_grad = product_right(node_pre_grad, node_weight_in)

    grad_scale = 1.0 / (nodes * patches * replicas)

    def by_patch(gradient):
        return (gradient * grad_scale).reshape(patches, -1, gradient.shape[1])

    readout = by_patch(product_left(updated, pred_grad))
    parts = width // readout.shape[2]
    short = readout.shape[1] // parts
    readout = jnp.concatenate([readout[:, i * short : (i + 1) * short] for i in range(parts)], axis=2)
    node_sums = reduce_rows(
        jnp.concatenate(
            [
                by_patch(product_left(node_input, node_pre_grad)),
                by_patch(product_left(node_hidden, node_z_grad)),
                readout,
            ],
            axis=1,
        )
    )

    aggregate_grad = input_grad[:, width:]
    high = aggregate_grad.astype(BF)
    low = (aggregate_grad - high.astype(F32)).astype(BF)
    gathered = product(jnp.concatenate([to_own, to_own], axis=1), jnp.concatenate([high, low], axis=0))
    message_grad = gathered * alive
    edge_z_grad = norm_back(message_grad, edge_normed, edge_inverse).astype(BF)
    edge_pre_grad = (product_right(edge_z_grad, edge_weight_out) * silu_grad(edge_pre)).astype(BF)

    halo_sum = product_left(from_halo, edge_pre_grad).astype(BF)
    returned = lax.all_to_all(
        halo_sum.reshape(patches, slots, width), "patch", split_axis=0, concat_axis=0, tiled=True
    ).reshape(patches * slots, width)
    sender_sum = product_left(from_own, edge_pre_grad)
    receiver_sum = product_left(to_own, edge_pre_grad).astype(BF)
    edge_sums = reduce_rows(
        jnp.concatenate(
            [
                by_patch(
                    jnp.concatenate(
                        [
                            product_left(node_rows, sender_sum.astype(BF)) + product_left(incoming, halo_sum),
                            product_left(node_rows, receiver_sum),
                            product_left(edge_rows, edge_pre_grad),
                        ],
                        axis=0,
                    )
                ),
                by_patch(product_left(edge_hidden, edge_z_grad)),
            ],
            axis=1,
        )
    )
    edge_result = product_right(edge_pre_grad, weight_e).astype(BF)
    total_sender = (sender_sum + product_left(pick, returned)).astype(BF)
    total = updated_grad + input_grad[:, :width]
    total = total + product_right(receiver_sum, weight_r) + product_right(total_sender, weight_s)

    edge_in_rows = edge_weight_in.shape[0] // patches
    node_in_rows = node_weight_in.shape[0] // patches
    node_out_rows = node_weight_out.shape[0] // patches
    tail = node_sums[node_in_rows + node_out_rows :]
    vars_width = readout_weight.shape[1]
    readout_grad = jnp.concatenate([tail[:, i * vars_width : (i + 1) * vars_width] for i in range(parts)], axis=0)
    return (
        total.astype(BF)[None],
        edge_result[None],
        edge_sums[:edge_in_rows],
        edge_sums[edge_in_rows:],
        node_sums[:node_in_rows],
        node_sums[node_in_rows : node_in_rows + node_out_rows],
        readout_grad,
    )


def solution(mesh):
    in_specs = (
        P("rep", "patch", None),
        P("rep", "patch", None),
        P("rep", "patch", None),
        P(),
        P(),
        P(),
        P(),
        P(),
        P("patch", None),
        P("patch", None),
        P("patch"),
        P("patch"),
        P("patch"),
        P("patch"),
        P("patch"),
    )
    out_specs = (
        P("rep", "patch", None),
        P("rep", "patch", None),
        P("patch", None),
        P("patch", None),
        P("patch", None),
        P("patch", None),
        P("patch", None),
    )
    return jax.shard_map(body, mesh=mesh, in_specs=in_specs, out_specs=out_specs, check_vma=False)
```

```python
import functools

import jax
import jax.numpy as jnp
from jax import lax
from jax.experimental import pallas as pl
from jax.experimental.pallas import tpu as pltpu
from jax.sharding import PartitionSpec as P

OCEAN = 32
BANDS = 721
OFFSETS = (1, -1, 2, -2, 3, -3)
LANES = 128
BLOCK = 1280
BF = jnp.bfloat16
F32 = jnp.float32
I32 = jnp.int32


def dot(left, right):
    return jnp.dot(left, right, preferred_element_type=F32)


def dot_left(left, right):
    return lax.dot_general(left, right, (((0,), (0,)), ((), ())), preferred_element_type=F32)


def dot_right(left, right):
    return lax.dot_general(left, right, (((1,), (1,)), ((), ())), preferred_element_type=F32)


def flipped(index, bits):
    out = 0
    for k in range(bits):
        out = out + ((index >> k) & 1) * (1 << (bits - 1 - k))
    return out


def bits_of(size):
    return size.bit_length() - 1


def column(row):
    return jnp.transpose(jnp.broadcast_to(row, (LANES, row.shape[1])))


def row_of(ref, at=slice(None)):
    return ref[at].reshape(1, -1)


def hot_rows(col, count):
    lane = lax.broadcasted_iota(I32, col.shape, 1)
    parts = [jnp.where(col == lane + at, 1.0, 0.0).astype(BF) for at in range(0, count, LANES)]
    return jnp.concatenate(parts, axis=1)


def hot_columns(row, count):
    ids = lax.broadcasted_iota(I32, (count, row.shape[1]), 0)
    return jnp.where(ids == row, 1.0, 0.0).astype(BF)


def silu_parts(values):
    logistic = 1.0 / (1.0 + jnp.exp(-values))
    return values * logistic, logistic * (1.0 + values * (1.0 - logistic))


def normalize(values):
    average = jnp.mean(values, axis=-1, keepdims=True)
    centred = values - average
    variance = jnp.mean(centred * centred, axis=-1, keepdims=True)
    inverse = lax.rsqrt(variance + 1e-05)
    return centred * inverse, inverse


def norm_back(gradient, normed, inverse):
    first = jnp.mean(gradient, axis=-1, keepdims=True)
    second = jnp.mean(gradient * normed, axis=-1, keepdims=True)
    return inverse * (gradient - first - normed * second)


def halo_index(sender, here, nodes, patches, slot, far, slots):
    beyond = sender - nodes
    k = sum((beyond >= j * slot).astype(I32) for j in range(1, 6))
    away = jnp.full_like(k, OFFSETS[0])
    for j in range(1, 6):
        away = jnp.where(k == j, OFFSETS[j], away)
    q = here - away
    q = jnp.where(q < 0, q + patches, q)
    q = jnp.where(q >= patches, q - patches, q)
    near_at = q * slots + beyond - k * slot
    distant = beyond - 6 * slot
    if far == 1:
        far_at = distant * slots + slot
    else:
        peer = sum((distant >= j * far).astype(I32) for j in range(1, patches))
        far_at = peer * slots + slot + distant - peer * far
    return jnp.where(beyond < 0, -1, jnp.where(beyond < 6 * slot, near_at, far_at))


class Fetched:
    def __init__(self, source, target, arrived):
        self.target = target
        self.copy = pltpu.make_async_copy(source, target, arrived)
        self.copy.start()

    def ready(self):
        if self.copy is not None:
            self.copy.wait()
            self.copy = None
        return self.target


class Stored:
    def __init__(self, source, target, arrived):
        self.source = source
        self.shape = source.shape
        self.dtype = source.dtype
        self.copy = pltpu.make_async_copy(source, target, arrived)
        self.sent = False

    def __getitem__(self, at):
        return self.source[at]

    def __setitem__(self, at, value):
        self.source[at] = value

    def send(self):
        if not self.sent:
            self.copy.start()
            self.sent = True


def pick_kernel(send, far_nodes, x, out_ref, *, patches, slot, far):
    out_ref[...] = jnp.zeros(out_ref.shape, out_ref.dtype)
    send_ref, far_ref, x_ref = send.ready(), far_nodes.ready(), x.ready()
    here = lax.axis_index("patch")
    nodes = x_ref.shape[0]
    near = dot_left(hot_columns(send_ref[...], nodes), x_ref[...]).astype(BF)
    distant = dot_left(hot_columns(far_ref[...], nodes), x_ref[...]).astype(BF)
    for k, offset in enumerate(OFFSETS):
        q = lax.rem(here + offset + patches, patches)
        out_ref[q, :slot, :] = near[k * slot : (k + 1) * slot]
    for q in range(patches):
        out_ref[q, slot : slot + far, :] = distant[q * far : (q + 1) * far]


def local_kernel(x, w, snd, rcv, e, pre_ref, table_ref):
    x_ref, w_ref = x.ready(), w.ready()
    nodes, width = x_ref.shape
    table_ref[:nodes] = dot(x_ref[...], w_ref[:width]).astype(BF)
    table_ref[nodes:] = dot(x_ref[...], w_ref[width : 2 * width]).astype(BF)
    snd_ref, rcv_ref, e_ref = snd.ready(), rcv.ready(), e.ready()

    def step(i, carry):
        at = pl.ds(pl.multiple_of(i * BLOCK, BLOCK), BLOCK)
        hot = jnp.concatenate(
            [hot_rows(column(row_of(snd_ref, at)), nodes), hot_rows(column(row_of(rcv_ref, at)), nodes)], axis=1
        )
        pre_ref[at] = dot(hot, table_ref[...]) + dot(e_ref[at], w_ref[2 * width :])
        return carry

    lax.fori_loop(0, e_ref.shape[0] // BLOCK, step, 0)


def place(full, out_ref, first_row, patches, patch_flip):
    rows = full.shape[0] // patches
    bits = bits_of(patches)
    for q in range(patches):
        out_ref[flipped(q, bits) ^ patch_flip, pl.ds(first_row, rows), :] = full[q * rows : (q + 1) * rows]


def order_lanes(values, out_ref, replicas, rep_flip, at=slice(None)):
    lanes = values.shape[1] // replicas
    bits = bits_of(replicas)
    for j in range(replicas):
        out_ref[flipped(j, bits) ^ rep_flip, at] = values[:, j * lanes : (j + 1) * lanes]


def lane_half(ref, upper, rows):
    half = ref.shape[0] // 2
    return jnp.concatenate([ref[i, :rows] for i in range(upper * half, (upper + 1) * half)], axis=1)


def forward_kernel(
    count_ref,
    w,
    halo_rows,
    snd,
    pre,
    out_w,
    rcv,
    x_rows,
    node_in,
    node_out,
    readout_w,
    target,
    land_nodes,
    bands,
    hidden_ref,
    slope_ref,
    message_ref,
    inverse_ref,
    base_ref,
    spread_ref,
    keep_ref,
    send_ref,
    part_ref,
    table_ref,
    order_ref,
    z_order_ref,
    tail_ref,
    *,
    patches,
    replicas,
    slot,
    far,
    slots,
):
    edges, width = hidden_ref.shape
    nodes = base_ref.shape[0]
    here = lax.axis_index("patch")
    halo = patches * slots
    padded = table_ref.shape[0]
    w_ref, halo_ref = w.ready(), halo_rows.ready()
    table_ref[:halo] = dot(halo_ref[...], w_ref[...]).astype(BF)
    if padded > halo:
        table_ref[halo:] = jnp.zeros((padded - halo, width), BF)
    live = count_ref[0]
    snd_ref, pre_ref, out_w_ref = snd.ready(), pre.ready(), out_w.ready()

    def step(i, carry):
        start = pl.multiple_of(i * BLOCK, BLOCK)
        at = pl.ds(start, BLOCK)
        place_of = halo_index(row_of(snd_ref, at), here, nodes, patches, slot, far, slots)
        total = pre_ref[at] + dot(hot_rows(column(place_of), padded), table_ref[...])
        hidden, slope = silu_parts(total)
        hidden = hidden.astype(BF)
        hidden_ref[at] = hidden
        slope_ref[at] = slope
        normed, inverse = normalize(dot(hidden, out_w_ref[...]))
        alive = lax.broadcasted_iota(I32, (BLOCK, 1), 0) + start < live
        message_ref[at] = jnp.where(alive, normed, 0.0).astype(BF)
        inverse_ref[at] = jnp.broadcast_to(jnp.where(alive, inverse, 0.0), (BLOCK, LANES))
        return carry

    lax.fori_loop(0, edges // BLOCK, step, 0)
    rcv_ref, x_ref, node_in_ref, node_out_ref = rcv.ready(), x_rows.ready(), node_in.ready(), node_out.ready()
    readout_ref, target_ref, land_ref, band_ref = readout_w.ready(), target.ready(), land_nodes.ready(), bands.ready()
    x = x_ref[...]
    aggregate = dot(hot_columns(row_of(rcv_ref), nodes), message_ref[...]).astype(BF)
    node_input = jnp.concatenate([x, aggregate], axis=1)
    node_hidden, node_slope = silu_parts(dot(node_input, node_in_ref[...]))
    node_hidden = node_hidden.astype(BF)
    node_normed, node_inverse = normalize(dot(node_hidden, node_out_ref[...]))
    updated = (x.astype(F32) + node_normed).astype(BF)
    predicted = dot(updated, readout_ref[...])
    band = column(row_of(band_ref)).astype(F32)
    area = jnp.cos(-0.5 * jnp.pi + (band + 0.5) * (jnp.pi / BANDS))[:, :1]
    land = column(row_of(land_ref))[:, :1]
    channel = lax.broadcasted_iota(I32, predicted.shape, 1)
    weight = jnp.where((channel < OCEAN) & (land == 1), 0.0, area)
    pred_grad = (weight * (predicted - target_ref[...].astype(F32))).astype(BF)
    updated_grad = dot_right(pred_grad, readout_ref[...])
    node_z_grad = norm_back(updated_grad, node_normed, node_inverse).astype(BF)
    node_pre_grad = (dot_right(node_z_grad, node_out_ref[...]) * node_slope).astype(BF)
    input_grad = dot_right(node_pre_grad, node_in_ref[...])
    base_ref[...] = updated_grad + input_grad[:, :width]
    base_ref.send()
    aggregate_grad = input_grad[:, width:]
    high = aggregate_grad.astype(BF)
    spread_ref[:nodes] = high
    spread_ref[nodes:] = (aggregate_grad - high.astype(F32)).astype(BF)

    patch_flip = flipped(here, bits_of(patches))
    rep_flip = flipped(lax.axis_index("rep"), bits_of(replicas))
    in_rows = 2 * width // patches
    out_rows = width // patches
    order_lanes(node_pre_grad, order_ref, replicas, rep_flip)
    place(dot_left(node_input, lane_half(order_ref, 0, nodes)), keep_ref, 0, patches, patch_flip)
    place(dot_left(node_input, lane_half(order_ref, 1, nodes)), part_ref, 0, patches, patch_flip)
    order_lanes(node_z_grad, z_order_ref, replicas, rep_flip)
    place(dot_left(node_hidden, lane_half(z_order_ref, 0, nodes)), keep_ref, in_rows, patches, patch_flip)
    place(dot_left(node_hidden, lane_half(z_order_ref, 1, nodes)), part_ref, in_rows, patches, patch_flip)
    readout = dot_left(updated, pred_grad)
    short = out_rows // replicas
    for q in range(patches):
        for j in range(replicas):
            at = q * out_rows + j * short
            tail_ref[flipped(j, bits_of(replicas)) ^ rep_flip, flipped(q, bits_of(patches)) ^ patch_flip] = readout[
                at : at + short
            ]
    half = replicas // 2
    rows = pl.ds(in_rows + out_rows, short)
    keep_ref[:, rows, :] = jnp.concatenate([tail_ref[i] for i in range(half)], axis=2)
    part_ref[:, rows, :] = jnp.concatenate([tail_ref[i] for i in range(half, replicas)], axis=2)
    send_ref[...] = part_ref[...].astype(BF)


def backward_kernel(
    slope_ref,
    message_ref,
    inverse_ref,
    spread_ref,
    out_w,
    rcv,
    snd,
    grad_ref,
    back_ref,
    own_ref,
    to_ref,
    order_ref,
    z_order_ref,
    sums_ref,
    to_sums_ref,
    *,
    patches,
    replicas,
    slot,
    far,
    slots,
):
    edges, width = grad_ref.shape
    nodes = own_ref.shape[0]
    halo = patches * slots
    here = lax.axis_index("patch")
    rep_flip = flipped(lax.axis_index("rep"), bits_of(replicas))
    out_w_ref, rcv_ref, snd_ref = out_w.ready(), rcv.ready(), snd.ready()

    def step(i, carry):
        at = pl.ds(pl.multiple_of(i * BLOCK, BLOCK), BLOCK)
        hot = hot_rows(column(row_of(rcv_ref, at)), nodes)
        message_grad = dot(jnp.concatenate([hot, hot], axis=1), spread_ref[...])
        z_grad = norm_back(message_grad, message_ref[at].astype(F32), inverse_ref[at][:, :1]).astype(BF)
        grad = (dot_right(z_grad, out_w_ref[...]) * slope_ref[at]).astype(BF)
        grad_ref[at] = grad
        order_lanes(grad, order_ref, replicas, rep_flip, at)
        order_lanes(z_grad, z_order_ref, replicas, rep_flip, at)
        return carry

    lax.fori_loop(0, edges // BLOCK, step, 0)
    grad_ref.send()
    grad = grad_ref[...]
    sender = row_of(snd_ref)
    place_of = halo_index(sender, here, nodes, patches, slot, far, slots)
    back = dot(hot_columns(place_of, halo), grad).astype(BF)
    back_ref[...] = back
    back_ref.send()
    own = dot(hot_columns(sender, nodes), grad)
    own_ref[...] = own
    own_ref.send()
    to = dot(hot_columns(row_of(rcv_ref), nodes), grad).astype(BF)
    to_ref[...] = to
    order_lanes(own.astype(BF), sums_ref, replicas, rep_flip, slice(0, nodes))
    order_lanes(back, sums_ref, replicas, rep_flip, slice(nodes, nodes + halo))
    order_lanes(to, to_sums_ref, replicas, rep_flip)


def weights_kernel(
    hidden_ref, z_order_ref, order_ref, sums_ref, to_sums_ref, e, x_rows, halo_rows, keep_ref, send_ref, part_ref, *, patches
):
    edges, width = hidden_ref.shape
    patch_flip = flipped(lax.axis_index("patch"), bits_of(patches))
    outs = ((0, keep_ref), (1, part_ref))
    in_rows = 3 * width // patches
    for upper, out_ref in outs:
        out_rows = dot_left(hidden_ref[...], lane_half(z_order_ref, upper, edges))
        place(out_rows, out_ref, in_rows, patches, patch_flip)
    e_ref, x_ref, halo_ref = e.ready(), x_rows.ready(), halo_rows.ready()
    nodes = x_ref.shape[0]
    halo = halo_ref.shape[0]
    for upper, out_ref in outs:
        sums = lane_half(sums_ref, upper, nodes + halo)
        sender_rows = dot_left(x_ref[...], sums[:nodes]) + dot_left(halo_ref[...], sums[nodes:])
        receiver_rows = dot_left(x_ref[...], lane_half(to_sums_ref, upper, nodes))
        edge_rows = dot_left(e_ref[...], lane_half(order_ref, upper, edges))
        place(jnp.concatenate([sender_rows, receiver_rows, edge_rows], axis=0), out_ref, 0, patches, patch_flip)
    send_ref[...] = part_ref[...].astype(BF)


def first_sum_kernel(keep_ref, other_ref, keep_a_ref, send_a_ref, keep_b_ref, send_b_ref):
    patches, first, lanes = keep_a_ref.shape
    half = patches // 2
    keep_a_ref[...] = keep_ref[:, :first, :lanes] + other_ref[:, :first, :lanes].astype(F32)
    send_a_ref[...] = (keep_ref[:, :first, lanes:] + other_ref[:, :first, lanes:].astype(F32)).astype(BF)
    keep_b_ref[...] = keep_ref[:half, first:, :] + other_ref[:half, first:, :].astype(F32)
    send_b_ref[...] = (keep_ref[half:, first:, :] + other_ref[half:, first:, :].astype(F32)).astype(BF)


def edge_kernel(base, to, w, grad, out_ref, total_ref):
    base_ref, to_ref, w_ref = base.ready(), to.ready(), w.ready()
    width = base_ref.shape[1]
    total_ref[...] = base_ref[...] + dot_right(to_ref[...], w_ref[width : 2 * width])
    out_ref[...] = dot_right(grad.ready()[...], w_ref[2 * width :]).astype(BF)


def node_kernel(back_rows, send, far_nodes, own_rows, w, total, out_ref, *, patches, slot, far):
    here = lax.axis_index("patch")
    back_ref, send_ref, far_ref = back_rows.ready(), send.ready(), far_nodes.ready()
    own_ref = own_rows.ready()
    nodes = own_ref.shape[0]
    near = []
    for k, offset in enumerate(OFFSETS):
        near.append(back_ref[lax.rem(here + offset + patches, patches), :slot, :])
    distant = [back_ref[q, slot : slot + far, :] for q in range(patches)]
    own = own_ref[...] + dot(hot_columns(send_ref[...], nodes), jnp.concatenate(near, axis=0))
    own = own + dot(hot_columns(far_ref[...], nodes), jnp.concatenate(distant, axis=0))
    out_ref[...] = (total.ready()[...] + dot_right(own.astype(BF), w.ready()[...])).astype(BF)


def finish_kernel(mine_ref, other_ref, pair_ref, *refs, replicas, scale, sections):
    outs, order_ref = refs[:-1], refs[-1]
    bits = bits_of(replicas)
    rep = lax.axis_index("rep")
    half = replicas // 2
    lanes = mine_ref.shape[1]
    blocks = [mine_ref, other_ref]
    for at in range(replicas):
        if at < half:
            value = blocks[at][...]
        else:
            value = pair_ref[at - half]
        order_ref[flipped(at, bits) ^ rep] = value.astype(F32) * scale
    start = 0
    for out_ref, (rows, folded) in zip(outs, sections):
        for j in range(replicas):
            value = order_ref[j, start : start + rows]
            if folded:
                out_ref[j * rows : (j + 1) * rows, :] = value
            else:
                out_ref[:, j * lanes : (j + 1) * lanes] = value
        start += rows


def swap(x, axis, mask):
    peers = lax.axis_size(axis)
    return lax.ppermute(x, axis, [(i, i ^ mask) for i in range(peers)])


def tied(values, others):
    values, _ = lax.optimization_barrier((values, others))
    return values


def reduce_start(keep, send):
    patches, rows, width = keep.shape
    first = max(rows // 2 // 16 * 16, min(8, rows // 2))
    shapes = ((patches, first, width // 2), (patches // 2, rows - first, width))
    outs = tuple(resident(shape, kind) for shape in shapes for kind in (F32, BF))
    return call(first_sum_kernel, outs, near=(0, 1))(keep, swap(send, "rep", 1))


def reduce_middle(parts):
    keep_a, send_a, keep_b, send_b = parts
    lanes = keep_a.shape[2]
    half = keep_b.shape[0]
    a = keep_a + swap(send_a, "rep", 2).astype(F32)
    b = keep_b + swap(send_b, "patch", 1).astype(F32)
    return a[:half], a[half:].astype(BF), b[..., :lanes], b[..., lanes:].astype(BF)


def reduce_end(parts):
    keep_a, send_a, keep_b, send_b = parts
    half = keep_a.shape[0]
    a = keep_a + swap(send_a, "patch", 1).astype(F32)
    b = keep_b + swap(send_b, "rep", 2).astype(F32)
    x = jnp.concatenate([a, b], axis=1)
    for k in range(1, bits_of(2 * half)):
        half //= 2
        x = x[:half] + swap(x[half:].astype(BF), "patch", 1 << k).astype(F32)
    return x[0].astype(BF)


def resident(shape, dtype):
    return pltpu.VMEM(shape, dtype)


def call(kernel, outs, scratch=(), smem=0, remote=None, near=(), limit=32, flops=0, **fixed):
    remote = remote or {}

    def run(*args):
        args = list(args)
        buffers = []
        specs = []
        for i, a in enumerate(args):
            if i < smem:
                specs.append(pl.BlockSpec(memory_space=pltpu.SMEM))
            elif i in remote:
                specs.append(pl.BlockSpec(memory_space=pltpu.HBM))
                args[i] = pltpu.with_memory_space_constraint(a, pltpu.HBM)
                buffers.append(pltpu.VMEM((remote[i] or a.shape[0], *a.shape[1:]), a.dtype))
            else:
                specs.append(pl.BlockSpec(memory_space=pltpu.VMEM))
                if i in near:
                    args[i] = pltpu.with_memory_space_constraint(a, pltpu.VMEM)
        count = len(args)
        held = len(buffers)
        single = not isinstance(outs, tuple)
        results = (outs,) if single else outs
        stored = [i for i, o in enumerate(results) if isinstance(o, jax.ShapeDtypeStruct)]
        places = [pl.BlockSpec(memory_space=pltpu.HBM if i in stored else pltpu.VMEM) for i in range(len(results))]
        shapes = tuple(pltpu.HBM(o.shape, o.dtype) if i in stored else o for i, o in enumerate(results))
        buffers += [pltpu.VMEM(results[i].shape, results[i].dtype) for i in stored]
        total = len(buffers)

        def wrapped(*refs):
            ins = list(refs[:count])
            made = list(refs[count : count + len(results)])
            rest = refs[count + len(results) :]
            if total:
                held_refs, arrived = rest[-total - 1 : -1], rest[-1]
                rest = rest[: -total - 1]
                for n, i in enumerate(sorted(remote)):
                    source = ins[i] if remote[i] is None else ins[i].at[pl.ds(0, remote[i])]
                    ins[i] = Fetched(source, held_refs[n], arrived.at[n])
                for n, i in enumerate(stored, held):
                    made[i] = Stored(held_refs[n], made[i], arrived.at[n])
            kernel(*ins, *made, *rest, **fixed)
            for value in ins:
                if isinstance(value, Fetched):
                    value.ready()
            for value in made:
                if isinstance(value, Stored):
                    value.send()
            for value in made:
                if isinstance(value, Stored):
                    value.copy.wait()

        extra = [*buffers, pltpu.SemaphoreType.DMA((total,))] if total else []
        moved = sum(a.size * a.dtype.itemsize for i, a in enumerate(args) if i not in near)
        done = pl.pallas_call(
            wrapped,
            out_shape=shapes,
            in_specs=specs,
            out_specs=tuple(places),
            scratch_shapes=[*scratch, *extra],
            compiler_params=pltpu.CompilerParams(vmem_limit_bytes=limit << 20),
            cost_estimate=pl.CostEstimate(flops=flops, bytes_accessed=moved, transcendentals=0),
            name=kernel.__name__,
        )(*args)
        return done[0] if single else done

    return run


def body(
    node_latents,
    edge_latents,
    targets,
    edge_weight_in,
    edge_weight_out,
    node_weight_in,
    node_weight_out,
    readout_weight,
    send_rows,
    far_rows,
    edge_sender,
    edge_receiver,
    edge_count,
    land_mask,
    lat_band,
):
    nodes, width = node_latents.shape[1:]
    edges = edge_latents.shape[1]
    patches = lax.axis_size("patch")
    replicas = lax.axis_size("rep")
    slot = send_rows.shape[1] // 6
    far = far_rows.shape[1] // patches
    slots = -(-(slot + far) // 8) * 8
    halo = patches * slots
    padded = -(-halo // LANES) * LANES
    lanes = width // replicas
    variables = readout_weight.shape[1]
    sds = jax.ShapeDtypeStruct
    sizes = dict(patches=patches, replicas=replicas, slot=slot, far=far, slots=slots)
    work = 2 * edges * width * width

    x = node_latents[0]
    e = edge_latents[0]
    outgoing = call(
        pick_kernel, sds((patches, slots, width), BF), remote=dict.fromkeys(range(3)), patches=patches, slot=slot, far=far
    )(send_rows, far_rows, x)
    incoming = lax.all_to_all(outgoing, "patch", split_axis=0, concat_axis=0, tiled=True).reshape(halo, width)
    local = call(
        local_kernel,
        sds((edges, width), F32),
        [pltpu.VMEM((2 * nodes, width), BF)],
        remote=dict.fromkeys(range(5)),
        flops=3 * work,
    )(x, edge_weight_in, edge_sender, edge_receiver, e)
    node_rows = (node_weight_in.shape[0] + node_weight_out.shape[0]) // patches + variables * width // patches // width
    half = replicas // 2 * lanes
    short = width // patches // replicas
    hidden, slope, message, inverse, base, spread, keep, send = call(
        forward_kernel,
        (
            resident((edges, width), BF),
            resident((edges, width), F32),
            resident((edges, width), BF),
            resident((edges, LANES), F32),
            sds((nodes, width), F32),
            resident((2 * nodes, width), BF),
            resident((patches, node_rows, half), F32),
            resident((patches, node_rows, half), BF),
        ),
        [
            pltpu.VMEM((patches, node_rows, half), F32),
            pltpu.VMEM((padded, width), BF),
            pltpu.VMEM((replicas, nodes, lanes), BF),
            pltpu.VMEM((replicas, nodes, lanes), BF),
            pltpu.VMEM((replicas, patches, short, variables), F32),
        ],
        smem=1,
        remote={**dict.fromkeys(range(1, 14)), 1: width},
        flops=4 * work,
        **sizes,
    )(
        edge_count,
        edge_weight_in,
        incoming,
        edge_sender,
        local,
        edge_weight_out,
        edge_receiver,
        x,
        node_weight_in,
        node_weight_out,
        readout_weight,
        targets[0],
        land_mask,
        lat_band,
    )
    node_parts = reduce_start(keep, send)
    edge_rows = (edge_weight_in.shape[0] + edge_weight_out.shape[0]) // patches
    ordered = resident((replicas, edges, lanes), BF)
    grad, back, own, to, order, z_order, sums, to_sums = call(
        backward_kernel,
        (
            sds((edges, width), BF),
            sds((halo, width), BF),
            sds((nodes, width), F32),
            sds((nodes, width), BF),
            ordered,
            ordered,
            resident((replicas, nodes + halo, lanes), BF),
            resident((replicas, nodes, lanes), BF),
        ),
        near=range(4),
        remote=dict.fromkeys(range(4, 7)),
        flops=4 * work,
        **sizes,
    )(slope, message, inverse, spread, edge_weight_out, edge_receiver, edge_sender)
    returned = lax.all_to_all(
        back.reshape(patches, slots, width), "patch", split_axis=0, concat_axis=0, tiled=True
    )
    sums = tied(sums, node_parts)
    keep, send = call(
        weights_kernel,
        (resident((patches, edge_rows, half), F32), resident((patches, edge_rows, half), BF)),
        [pltpu.VMEM((patches, edge_rows, half), F32)],
        near=range(5),
        remote=dict.fromkeys(range(5, 8)),
        flops=3 * work,
        patches=patches,
    )(hidden, z_order, order, sums, to_sums, e, x, incoming)
    node_parts = reduce_middle(node_parts)
    edge_parts = reduce_start(keep, send)
    edge_result, total = call(
        edge_kernel,
        (sds((edges, width), BF), sds((nodes, width), F32)),
        remote=dict.fromkeys(range(4)),
        flops=2 * work,
    )(base, to, edge_weight_in, grad)
    edge_parts = reduce_middle(edge_parts)
    edge_parts = tied(edge_parts, (edge_result, returned))
    node_result = call(
        node_kernel,
        sds((nodes, width), BF),
        remote={**dict.fromkeys(range(6)), 4: width},
        flops=work,
        patches=patches,
        slot=slot,
        far=far,
    )(returned, send_rows, far_rows, own, edge_weight_in, total)
    node_sums = reduce_end(node_parts)
    edge_sums = reduce_end(edge_parts)

    mine = jnp.concatenate([edge_sums, node_sums], axis=0)
    other = swap(mine, "rep", 2)
    pair = swap(jnp.stack([mine, other]), "rep", 1)
    sections = (
        (edge_weight_in.shape[0] // patches, False),
        (edge_weight_out.shape[0] // patches, False),
        (node_weight_in.shape[0] // patches, False),
        (node_weight_out.shape[0] // patches, False),
        (short, True),
    )
    outs = tuple(
        sds((rows * replicas, variables) if folded else (rows, width), F32) for rows, folded in sections
    )
    grads = call(
        finish_kernel,
        outs,
        [pltpu.VMEM((replicas, edge_rows + node_rows, lanes), F32)],
        replicas=replicas,
        scale=1.0 / (nodes * patches * replicas),
        sections=sections,
    )(mine, other, pair)
    return (node_result[None], edge_result[None], *grads)


def solution(mesh):
    in_specs = (
        P("rep", "patch", None),
        P("rep", "patch", None),
        P("rep", "patch", None),
        P(),
        P(),
        P(),
        P(),
        P(),
        P("patch", None),
        P("patch", None),
        P("patch"),
        P("patch"),
        P("patch"),
        P("patch"),
        P("patch"),
    )
    out_specs = (
        P("rep", "patch", None),
        P("rep", "patch", None),
        P("patch", None),
        P("patch", None),
        P("patch", None),
        P("patch", None),
        P("patch", None),
    )
    return jax.shard_map(body, mesh=mesh, in_specs=in_specs, out_specs=out_specs, check_vma=False)
```
